32 devices in a mesh: rep: 8 (over z, y), fsdp: 4 (over x, core).
Axes of the slice: x: 2, y: 2, z: 4, core: 2. Of those that a mesh axis runs over, the one named last changes fastest.
Arguments:
- gradients: bfloat16 [8, 4, 1024, 2048], P('rep', 'fsdp'), may hold values from -6 to 6
- momentum: float32 [8, 1024, 2048], P('rep', None, 'fsdp'), may hold values from -12 to 12
- master_weights: float32 [1024, 2048], P(None, 'fsdp'), may hold values from -0.125 to 0.125
Outputs:
- new_momentum: float32 [8, 1024, 2048], P('rep', None, 'fsdp')
- new_master: float32 [1024, 2048], P(None, 'fsdp')
- weights_full: bfloat16 [1024, 2048], replicated
The draws below stay inside these ranges and needn't reach their ends.
All inputs are finite; a program needn't handle non-finite values.
Results may differ from the reference program's by a relative error of at most 0.012.
Values may be sent and summed in bfloat16 or wider, within the bound.
A program may use at most 128 MiB of HBM per device.

```python
import jax
import jax.numpy as jnp
from jax import lax

D = 2048
ROWS = 1024
GROUP = 128
BAND = 16
REPS = 8
SHARDS = 4


def with_spikes(array, rng, source, target, parts, factor):
    owner, partner = [(jnp.arange(array.shape[axis_at]) // (array.shape[axis_at] // parts)).reshape([-1 if axis == axis_at else 1 for axis in range(array.ndim)]) for axis_at in (source, target)]
    chosen = jax.random.permutation(rng, parts)[partner]
    strong = (owner == chosen) | (owner == (partner + parts // 2) % parts)
    return jnp.where(strong, factor * array, array)


def level_of(stream_key, extent, split, smallest, high):
    gain, own = 1.0, jax.random.fold_in(stream_key, 6)
    for position, parts in split:
        draws = jnp.exp(jax.random.uniform(jax.random.fold_in(own, position), (parts,), jnp.float32, smallest / len(split), high / len(split)))
        gain = gain * jnp.repeat(draws, extent[position] // parts).reshape([-1 if axis == position else 1 for axis in range(len(extent))])
    return gain


def normal_values(stream_key, dims, width, bound, pieces=(), kind=jnp.bfloat16):
    gain = level_of(stream_key, dims, pieces, -0.22, 0.18) if pieces else 1.0
    entries = jax.random.normal(stream_key, dims, jnp.float32) * width * gain
    return jnp.minimum(jnp.maximum(entries, -bound), bound).astype(kind)


def noise_with(stream_key, extent, scale, most, cuts, heavy, kind=jnp.bfloat16):
    entries = scale * jax.random.normal(stream_key, extent, jnp.float32)
    if cuts:
        entries = entries * level_of(stream_key, extent, cuts, -0.22, 0.18)
    return jnp.clip(with_spikes(entries, jax.random.fold_in(stream_key, 3), *heavy), -most, most).astype(kind)


def setup_inputs(seed: int = 0) -> dict:
    seeds = jax.random.split(jax.random.key(seed), 4)
    gradients = noise_with(seeds[0], (REPS, SHARDS, ROWS, D), 1.0, 6.0, ((0, 8), (1, 4)), (1, 3, 4, 2.0))
    momentum = normal_values(seeds[1], (REPS, ROWS, D), 2.0, 12.0, ((0, 8), (2, 4)), jnp.float32)
    master_weights = normal_values(seeds[2], (ROWS, D), D ** -0.5, 0.125, ((1, 4),), jnp.float32)
    return {"gradients": gradients, "momentum": momentum, "master_weights": master_weights}


momentum_decay = 0.9
step_size = 0.05

def cosine_rows():
    freq = jnp.arange(BAND, dtype=jnp.float32)[:, None]
    place = jnp.arange(GROUP, dtype=jnp.float32)[None, :]
    factor = jnp.where(freq == 0.0, jnp.sqrt(1.0 / GROUP), jnp.sqrt(2.0 / GROUP)).astype(jnp.float32)
    return (factor * jnp.cos(jnp.pi * (2.0 * place + 1.0) * freq / (2.0 * GROUP))).astype(jnp.float32)

def band_of(matrix):
    table = cosine_rows()
    blocks = matrix.reshape(matrix.shape[0] // GROUP, GROUP, matrix.shape[1] // GROUP, GROUP)
    return jnp.einsum('kr,arbc,lc->abkl', table, blocks, table, precision=lax.Precision.HIGHEST)

def spread_band(coeffs):
    table = cosine_rows()
    blocks = jnp.einsum('kr,abkl,lc->arbc', table, coeffs, table, precision=lax.Precision.HIGHEST)
    return blocks.reshape(coeffs.shape[0] * GROUP, coeffs.shape[1] * GROUP)

def one_replica(inputs):
    partial_grads, moment_old = inputs
    summed = lax.optimization_barrier(jnp.sum(partial_grads.astype(jnp.float32), axis=0))
    moment = momentum_decay * moment_old + summed
    band = band_of(moment)
    return (moment - spread_band(band), band)

def reference(gradients, momentum, master_weights):
    new_momentum, bands = lax.map(one_replica, (gradients, momentum))
    mean_band = lax.optimization_barrier(jnp.sum(bands, axis=0)) / REPS
    new_master = master_weights - step_size * spread_band(mean_band)
    return (new_momentum, new_master, new_master.astype(jnp.bfloat16))
```

```python
import functools

import jax
import jax.numpy as jnp
import numpy as np
from jax import lax
from jax.experimental import pallas as pl
from jax.experimental.pallas import tpu as pltpu
from jax.sharding import PartitionSpec as P

GROUP = 128
BAND = 16
LANES = 128
HALF = LANES // 2

momentum_decay = 0.9
step_size = 0.05

MESH = pl.DeviceIdType.MESH


def cosine_rows():
    freq = np.arange(BAND, dtype=np.float64)[:, None]
    place = np.arange(GROUP, dtype=np.float64)[None, :]
    factor = np.where(freq == 0.0, np.sqrt(1.0 / GROUP), np.sqrt(2.0 / GROUP))
    return factor * np.cos(np.pi * (2.0 * place + 1.0) * freq / (2.0 * GROUP))


def tables(width):
    rows = cosine_rows()
    blocks = width // GROUP
    spread = np.zeros((HALF, width))
    for b in range(blocks):
        spread[b * BAND : (b + 1) * BAND, b * GROUP : (b + 1) * GROUP] = rows
    return rows, np.concatenate([spread, spread], axis=0)


def split(values):
    values = jnp.asarray(values, jnp.float32)
    high = values.astype(jnp.bfloat16)
    return high, (values - high.astype(jnp.float32)).astype(jnp.bfloat16)


def high_low(both):
    high = both.astype(jnp.bfloat16).astype(jnp.float32)
    lane = lax.broadcasted_iota(jnp.int32, both.shape, 1)
    return jnp.where(lane < HALF, high, both - high).astype(jnp.bfloat16)


def batches(chunks):
    if chunks < 4:
        return [(0, chunks)]
    return [(0, chunks // 2), (chunks // 2, chunks - 1), (chunks - 1, chunks)]


def exchange(
    nr, nf, grads, momentum, master, lrows, lcols,
    moment_out, raw_out, own_out, mean_out,
    gbuf, pbuf, sbuf, rbuf, mom, mout, mas, mcast, wland, bands, means,
    g_sem, mom_sem, mas_sem, mout_sem, raw_sem, own_sem, mean_sem,
    p_send, p_recv, x_send, x_recv, c_send, c_recv, m_send, m_recv,
    w_send, w_recv, f_send, f_recv, b_send, b_recv, e_send, e_recv,
):
    r, f = lax.axis_index("rep"), lax.axis_index("fsdp")
    pairs = nf // 2
    core = lax.rem(f, 2)
    pair = f // 2
    other = 1 - core
    partner = (r, pair * 2 + other)
    rows, width = momentum.shape[1], momentum.shape[2]
    chunks = rows // GROUP
    share = rows // nr
    mine = pl.ds(pl.multiple_of(r * share, share), share)

    def columns(block):
        return pl.ds(pl.multiple_of(block * width, width), width)

    mas_first = pltpu.make_async_copy(master.at[mine], mas.at[mine], mas_sem.at[0])
    mas_first.start()
    g_copies = []
    for i in range(chunks):
        at = pl.ds(i * GROUP, GROUP)
        for s in range(pairs):
            q = lax.rem(pair + s, pairs)
            c = pltpu.make_async_copy(
                grads.at[0, 0, at, columns(q * 2 + core)], gbuf.at[i, s], g_sem.at[i, s]
            )
            c.start()
            g_copies.append(c)

    barrier = pltpu.get_barrier_semaphore()
    for s in range(1, nr):
        pl.semaphore_signal(barrier, inc=1, device_id=(lax.rem(r + s, nr), f), device_id_type=MESH)
    for s in range(1, nf):
        pl.semaphore_signal(barrier, inc=1, device_id=(r, lax.rem(f + s, nf)), device_id_type=MESH)
    pl.semaphore_wait(barrier, nr - 1 + nf - 1)

    def remote(src, dst, send, recv, to):
        return pltpu.make_async_remote_copy(
            src_ref=src, dst_ref=dst, send_sem=send, recv_sem=recv, device_id=to, device_id_type=MESH
        )

    p_copies = []
    for i in range(chunks):
        at = pl.ds(i * GROUP, GROUP)
        for s in list(range(1, pairs)) + [0]:
            q = lax.rem(pair + s, pairs)
            c = remote(
                grads.at[0, 0, at, columns(q * 2 + other)], pbuf.at[i, s],
                p_send.at[i, s], p_recv.at[i, s], partner,
            )
            c.start()
            p_copies.append(c)

    mom_copies = []
    for i in range(chunks):
        at = pl.ds(i * GROUP, GROUP)
        c = pltpu.make_async_copy(momentum.at[0, at], mom.at[at], mom_sem.at[i])
        c.start()
        mom_copies.append(c)
    mas_all = pltpu.make_async_copy(master, mas.at[pl.ds(rows, rows)], mas_sem.at[1])
    mas_all.start()

    mas_first.wait()
    mcast[pl.ds(rows, share)] = mas[mine].astype(jnp.bfloat16)
    c_copies = []
    for s in range(1, pairs):
        q = lax.rem(pair + s, pairs)
        c = remote(
            mcast.at[pl.ds(rows, share)], wland.at[pairs - s - 1, mine],
            c_send.at[s - 1], c_recv.at[pairs - s - 1], (r, q * 2 + core),
        )
        c.start()
        c_copies.append(c)


    def g_at(i, s):
        return g_copies[i * pairs + s]

    def p_at(i, s):
        order = list(range(1, pairs)) + [0]
        return p_copies[i * pairs + order.index(s)]

    x_copies = []
    for i in range(chunks):
        for s in range(1, pairs):
            q = lax.rem(pair + s, pairs)
            g_at(i, s).wait()
            p_at(i, s).wait()
            sbuf[i, s - 1] = (
                gbuf[i, s].astype(jnp.float32) + pbuf[i, s].astype(jnp.float32)
            ).astype(jnp.bfloat16)
            c = remote(
                sbuf.at[i, s - 1], rbuf.at[i, pairs - s - 1],
                x_send.at[i, s - 1], x_recv.at[i, pairs - s - 1], (r, q * 2 + core),
            )
            c.start()
            x_copies.append((i, s, c))
        if i == chunks // 2 - 1:
            for s in range(pairs - 1):
                c_copies[pairs - 2 - s].wait_recv()
            w_copies = []
            for t in range(1, nr):
                for s in range(pairs - 1):
                    c = remote(
                        wland.at[s, mine], wland.at[s, mine],
                        w_send.at[s, t - 1], w_recv.at[s, nr - t - 1], (lax.rem(r + t, nr), f),
                    )
                    c.start()
                    w_copies.append(c)
    mas_all.wait()
    mcast[pl.ds(0, rows)] = mas[pl.ds(rows, rows)].astype(jnp.bfloat16)
    m_copy = remote(mcast.at[pl.ds(0, rows)], raw_out.at[f], m_send, m_recv, partner)
    m_copy.start()

    b_copies = []
    local = []
    for first, last in batches(chunks):
        for i in range(first, last):
            at = pl.ds(i * GROUP, GROUP)
            g_at(i, 0).wait()
            p_at(i, 0).wait()
            mom_copies[i].wait()
            total = gbuf[i, 0].astype(jnp.float32) + pbuf[i, 0].astype(jnp.float32)
            for j, s, c in x_copies:
                if j == i:
                    c.wait_recv()
            for s in range(pairs - 1):
                total = total + rbuf[i, s].astype(jnp.float32)
            moment = momentum_decay * mom[at] + total
            mout[at] = moment
            c = pltpu.make_async_copy(mout.at[at], moment_out.at[at], mout_sem.at[i])
            c.start()
            local.append(c)
            half = jnp.dot(
                lrows[...], moment, precision=lax.Precision.HIGHEST, preferred_element_type=jnp.float32
            )
            both = jnp.dot(
                half, lcols[...], precision=lax.Precision.HIGHEST, preferred_element_type=jnp.float32
            )
            bands[0, pl.ds(i * BAND, BAND)] = high_low(both)
        part = pl.ds(first * BAND, (last - first) * BAND)
        n = batches(chunks).index((first, last))
        for t in range(1, nr):
            c = remote(
                bands.at[0, part], bands.at[nr - t, part],
                b_send.at[n, t - 1], b_recv.at[n, nr - t - 1], (lax.rem(r + t, nr), f),
            )
            c.start()
            b_copies.append(c)
    c = pltpu.make_async_copy(bands.at[0], own_out, own_sem)
    c.start()
    local.append(c)

    for c in w_copies:
        c.wait_recv()
    f_copies = []
    for s in range(pairs - 1):
        q = lax.rem(pair + s + 1, pairs)
        c = remote(wland.at[s], raw_out.at[q * 2 + core], f_send.at[s], f_recv.at[s], partner)
        c.start()
        f_copies.append(c)
        c = pltpu.make_async_copy(wland.at[s], raw_out.at[q * 2 + core], raw_sem.at[s])
        c.start()
        local.append(c)

    for c in b_copies:
        c.wait_recv()
    total = bands[0].astype(jnp.float32)
    for t in range(1, nr):
        total = total + bands[t].astype(jnp.float32)
    means[0] = high_low((total + pltpu.roll(total, HALF, 1)) * (1.0 / nr))
    e_copies = []
    for t in range(1, nf):
        c = remote(
            means.at[0], mean_out.at[f], e_send.at[t - 1], e_recv.at[nf - t - 1],
            (r, lax.rem(f + t, nf)),
        )
        c.start()
        e_copies.append(c)
    c = pltpu.make_async_copy(means.at[0], mean_out.at[f], mean_sem)
    c.start()
    local.append(c)

    for c in local:
        c.wait()
    for c in c_copies + w_copies + b_copies + [c for _, _, c in x_copies]:
        c.wait_send()
    m_copy.wait()
    for c in f_copies + e_copies:
        c.wait()


def finish(nf, moment, master, raw, own, mean, thigh, tlow, left, f_ref, momentum_out, master_out, full_out):
    width = master.shape[1]
    f = f_ref[0]

    def spread(coeffs):
        half = jnp.dot(coeffs, thigh[...], preferred_element_type=jnp.float32)
        half = half + jnp.dot(coeffs, tlow[...], preferred_element_type=jnp.float32)
        high = half.astype(jnp.bfloat16)
        low = (half - high.astype(jnp.float32)).astype(jnp.bfloat16)
        return jnp.dot(
            left[...], jnp.concatenate([high, high, low], axis=0), preferred_element_type=jnp.float32
        )

    momentum_out[0] = moment[...] - spread(own[...])
    for j in range(nf):
        full_out[:, j * width : (j + 1) * width] = (
            raw[j].astype(jnp.float32) - step_size * spread(mean[j])
        ).astype(jnp.bfloat16)
    new_master = master[...] - step_size * spread(mean[f])
    master_out[...] = new_master
    full_out[:, pl.ds(pl.multiple_of(f * width, width), width)] = new_master.astype(jnp.bfloat16)


def local(nr, nf, gradients, momentum, master_weights):
    rows, width = master_weights.shape
    chunks = rows // GROUP
    pairs = nf // 2
    table, twice = tables(width)
    thigh, tlow = split(twice)
    lhigh, llow = split(table.T)
    left = jnp.concatenate([lhigh, llow, lhigh], axis=1)
    anywhere = pl.BlockSpec(memory_space=pl.ANY)
    vmem = pl.BlockSpec(memory_space=pltpu.VMEM)
    dma = pltpu.SemaphoreType.DMA
    bf16, f32 = jnp.bfloat16, jnp.float32
    nb = len(batches(chunks))
    share = rows // nr
    moment, raw, own, mean = pl.pallas_call(
        functools.partial(exchange, nr, nf),
        out_shape=(
            jax.ShapeDtypeStruct((rows, width), f32),
            jax.ShapeDtypeStruct((nf, rows, width), bf16),
            jax.ShapeDtypeStruct((chunks * BAND, LANES), bf16),
            jax.ShapeDtypeStruct((nf, chunks * BAND, LANES), bf16),
        ),
        in_specs=[anywhere, anywhere, anywhere, vmem, vmem],
        out_specs=(anywhere,) * 4,
        scratch_shapes=[
            pltpu.VMEM((chunks, pairs, GROUP, width), bf16),
            pltpu.VMEM((chunks, pairs, GROUP, width), bf16),
            pltpu.VMEM((chunks, pairs - 1, GROUP, width), bf16),
            pltpu.VMEM((chunks, pairs - 1, GROUP, width), bf16),
            pltpu.VMEM((rows, width), f32),
            pltpu.VMEM((rows, width), f32),
            pltpu.VMEM((2 * rows, width), f32),
            pltpu.VMEM((rows + share, width), bf16),
            pltpu.VMEM((pairs - 1, rows, width), bf16),
            pltpu.VMEM((nr, chunks * BAND, LANES), bf16),
            pltpu.VMEM((1, chunks * BAND, LANES), bf16),
            dma((chunks, pairs)),
            dma((chunks,)),
            dma((2,)),
            dma((chunks,)),
            dma((pairs - 1,)),
            dma,
            dma,
            dma((chunks, pairs)),
            dma((chunks, pairs)),
            dma((chunks, pairs - 1)),
            dma((chunks, pairs - 1)),
            dma((pairs - 1,)),
            dma((pairs - 1,)),
            dma,
            dma,
            dma((pairs - 1, nr - 1)),
            dma((pairs - 1, nr - 1)),
            dma((pairs - 1,)),
            dma((pairs - 1,)),
            dma((nb, nr - 1)),
            dma((nb, nr - 1)),
            dma((nf - 1,)),
            dma((nf - 1,)),
        ],
        compiler_params=pltpu.CompilerParams(
            collective_id=0, has_side_effects=True, vmem_limit_bytes=40 * 1024 * 1024
        ),
        name="exchange",
    )(gradients, momentum, master_weights, jnp.asarray(table, f32), jnp.asarray(twice.T, f32))

    def whole(shape):
        return pl.BlockSpec(shape, lambda a: (0,) * len(shape))

    return pl.pallas_call(
        functools.partial(finish, nf),
        grid=(chunks,),
        out_shape=(
            jax.ShapeDtypeStruct((1, rows, width), f32),
            jax.ShapeDtypeStruct((rows, width), f32),
            jax.ShapeDtypeStruct((rows, nf * width), bf16),
        ),
        in_specs=[
            pl.BlockSpec((GROUP, width), lambda a: (a, 0)),
            pl.BlockSpec((GROUP, width), lambda a: (a, 0)),
            pl.BlockSpec((nf, GROUP, width), lambda a: (0, a, 0)),
            pl.BlockSpec((BAND, LANES), lambda a: (a, 0)),
            pl.BlockSpec((nf, BAND, LANES), lambda a: (0, a, 0)),
            whole((LANES, width)),
            whole((LANES, width)),
            whole((GROUP, 3 * BAND)),
            pl.BlockSpec(memory_space=pltpu.SMEM),
        ],
        out_specs=(
            pl.BlockSpec((1, GROUP, width), lambda a: (0, a, 0)),
            pl.BlockSpec((GROUP, width), lambda a: (a, 0)),
            pl.BlockSpec((GROUP, nf * width), lambda a: (a, 0)),
        ),
        name="finish",
    )(moment, master_weights, raw, own, mean, thigh, tlow, left, lax.axis_index("fsdp").astype(jnp.int32)[None])


def solution(mesh):
    return jax.shard_map(
        functools.partial(local, mesh.shape["rep"], mesh.shape["fsdp"]),
        mesh=mesh,
        in_specs=(P("rep", "fsdp", None, None), P("rep", None, "fsdp"), P(None, "fsdp")),
        out_specs=(P("rep", None, "fsdp"), P(None, "fsdp"), P()),
        check_vma=False,
    )
```

```python
import functools

import jax
import jax.numpy as jnp
import numpy as np
from jax import lax
from jax.experimental import pallas as pl
from jax.experimental.pallas import tpu as pltpu
from jax.sharding import PartitionSpec as P

GROUP = 128
BAND = 16
LANES = 128
HALF = LANES // 2

momentum_decay = 0.9
step_size = 0.05

MESH = pl.DeviceIdType.MESH


def cosine_rows():
    freq = np.arange(BAND, dtype=np.float64)[:, None]
    place = np.arange(GROUP, dtype=np.float64)[None, :]
    factor = np.where(freq == 0.0, np.sqrt(1.0 / GROUP), np.sqrt(2.0 / GROUP))
    return factor * np.cos(np.pi * (2.0 * place + 1.0) * freq / (2.0 * GROUP))


def tables(width):
    rows = cosine_rows()
    blocks = width // GROUP
    spread = np.zeros((HALF, width))
    for b in range(blocks):
        spread[b * BAND : (b + 1) * BAND, b * GROUP : (b + 1) * GROUP] = rows
    return rows, np.concatenate([spread, spread], axis=0)


def split(values):
    values = jnp.asarray(values, jnp.float32)
    high = values.astype(jnp.bfloat16)
    return high, (values - high.astype(jnp.float32)).astype(jnp.bfloat16)


def high_low(both):
    high = both.astype(jnp.bfloat16).astype(jnp.float32)
    lane = lax.broadcasted_iota(jnp.int32, both.shape, 1)
    return jnp.where(lane < HALF, high, both - high).astype(jnp.bfloat16)


def spread_half(coeffs, thigh, tlow):
    half = jnp.dot(coeffs, thigh[...], preferred_element_type=jnp.float32)
    return half + jnp.dot(coeffs, tlow[...], preferred_element_type=jnp.float32)


def batches(chunks):
    if chunks < 4:
        return [(0, chunks)]
    return [(0, chunks // 2), (chunks // 2, chunks - 1), (chunks - 1, chunks)]


def exchange(
    nr, nf, grads, momentum, master, *rest
):
    hbm_tables, rest = rest[:6], rest[6:]
    (
    moment_out, raw_out, mean_out,
    gbuf, pbuf, sbuf, rbuf, mom, mout, mas, mcast, wland, bands, means,
    g_sem, mom_sem, mas_sem, mout_sem, raw_sem, mean_sem,
    p_send, p_recv, x_send, x_recv, c_send, c_recv, m_send, m_recv,
    w_send, w_recv, f_send, f_recv, b_send, b_recv, e_send, e_recv,
    t_sem, *vmem_tables,
    ) = rest
    lboth, chigh, clow, thigh, tlow, left = vmem_tables
    r, f = lax.axis_index("rep"), lax.axis_index("fsdp")
    pairs = nf // 2
    core = lax.rem(f, 2)
    pair = f // 2
    other = 1 - core
    partner = (r, pair * 2 + other)
    rows, width = momentum.shape[1], momentum.shape[2]
    chunks = rows // GROUP
    share = rows // nr
    mine = pl.ds(pl.multiple_of(r * share, share), share)

    def columns(block):
        return pl.ds(pl.multiple_of(block * width, width), width)

    mas_first = pltpu.make_async_copy(master.at[mine], mas.at[mine], mas_sem.at[0])
    mas_first.start()
    g_copies = []
    for i in range(chunks):
        at = pl.ds(i * GROUP, GROUP)
        for s in range(pairs):
            q = lax.rem(pair + s, pairs)
            c = pltpu.make_async_copy(
                grads.at[0, 0, at, columns(q * 2 + core)], gbuf.at[i, s], g_sem.at[i, s]
            )
            c.start()
            g_copies.append(c)

    t_copies = []
    for n, (src, dst) in enumerate(zip(hbm_tables, vmem_tables)):
        c = pltpu.make_async_copy(src, dst, t_sem.at[n])
        c.start()
        t_copies.append(c)

    barrier = pltpu.get_barrier_semaphore()
    for s in range(1, nr):
        pl.semaphore_signal(barrier, inc=1, device_id=(lax.rem(r + s, nr), f), device_id_type=MESH)
    for s in range(1, nf):
        pl.semaphore_signal(barrier, inc=1, device_id=(r, lax.rem(f + s, nf)), device_id_type=MESH)
    pl.semaphore_wait(barrier, nr - 1 + nf - 1)

    def remote(src, dst, send, recv, to):
        return pltpu.make_async_remote_copy(
            src_ref=src, dst_ref=dst, send_sem=send, recv_sem=recv, device_id=to, device_id_type=MESH
        )

    p_copies = []
    order = [(i, s) for i in range(chunks) for s in range(1, pairs)] + [(i, 0) for i in range(chunks)]
    for i, s in order:
        at = pl.ds(i * GROUP, GROUP)
        q = lax.rem(pair + s, pairs)
        c = remote(
            grads.at[0, 0, at, columns(q * 2 + other)], pbuf.at[i, s],
            p_send.at[i, s], p_recv.at[i, s], partner,
        )
        c.start()
        p_copies.append(c)

    mom_copies = []
    for i in range(chunks):
        at = pl.ds(i * GROUP, GROUP)
        c = pltpu.make_async_copy(momentum.at[0, at], mom.at[at], mom_sem.at[i])
        c.start()
        mom_copies.append(c)
    mas_all = pltpu.make_async_copy(master, mas.at[pl.ds(rows, rows)], mas_sem.at[1])
    mas_all.start()

    mas_first.wait()
    mcast[pl.ds(rows, share)] = mas[mine].astype(jnp.bfloat16)
    c_copies = []
    for s in range(1, pairs):
        q = lax.rem(pair + s, pairs)
        c = remote(
            mcast.at[pl.ds(rows, share)], wland.at[pairs - s - 1, mine],
            c_send.at[s - 1], c_recv.at[pairs - s - 1], (r, q * 2 + core),
        )
        c.start()
        c_copies.append(c)


    def g_at(i, s):
        return g_copies[i * pairs + s]

    def p_at(i, s):
        return p_copies[order.index((i, s))]

    x_copies = []
    for i in range(chunks):
        for s in range(1, pairs):
            q = lax.rem(pair + s, pairs)
            g_at(i, s).wait()
            p_at(i, s).wait()
            sbuf[i, s - 1] = (
                gbuf[i, s].astype(jnp.float32) + pbuf[i, s].astype(jnp.float32)
            ).astype(jnp.bfloat16)
            c = remote(
                sbuf.at[i, s - 1], rbuf.at[i, pairs - s - 1],
                x_send.at[i, s - 1], x_recv.at[i, pairs - s - 1], (r, q * 2 + core),
            )
            c.start()
            x_copies.append((i, s, c))
        if i == chunks // 2 - 1:
            for s in range(pairs - 1):
                c_copies[pairs - 2 - s].wait_recv()
            w_copies = []
            for t in range(1, nr):
                for s in range(pairs - 1):
                    c = remote(
                        wland.at[s, mine], wland.at[s, mine],
                        w_send.at[s, t - 1], w_recv.at[s, nr - t - 1], (lax.rem(r + t, nr), f),
                    )
                    c.start()
                    w_copies.append(c)
    mas_all.wait()
    mcast[pl.ds(0, rows)] = mas[pl.ds(rows, rows)].astype(jnp.bfloat16)
    m_copy = remote(mcast.at[pl.ds(0, rows)], raw_out.at[f], m_send, m_recv, partner)
    m_copy.start()

    for c in t_copies:
        c.wait()

    b_copies = []
    local = []

    def take_out(i):
        at = pl.ds(i * GROUP, GROUP)
        half = spread_half(bands[0, pl.ds(i * BAND, BAND)], thigh, tlow)
        high, low = split(half)
        mout[at] = mom[at] - jnp.dot(
            left[...], jnp.concatenate([high, high, low], axis=0), preferred_element_type=jnp.float32
        )
        c = pltpu.make_async_copy(mout.at[at], moment_out.at[0, at], mout_sem.at[i])
        c.start()
        local.append(c)

    for first, last in batches(chunks):
        for i in range(first, last):
            at = pl.ds(i * GROUP, GROUP)
            g_at(i, 0).wait()
            p_at(i, 0).wait()
            mom_copies[i].wait()
            total = gbuf[i, 0].astype(jnp.float32) + pbuf[i, 0].astype(jnp.float32)
            for j, s, c in x_copies:
                if j == i:
                    c.wait_recv()
            for s in range(pairs - 1):
                total = total + rbuf[i, s].astype(jnp.float32)
            moment = momentum_decay * mom[at] + total
            mom[at] = moment
            high, low = split(moment)
            first_part = jnp.dot(lboth[...], high, preferred_element_type=jnp.float32)
            half = first_part[:BAND] + first_part[BAND:] + jnp.dot(
                lboth[...], low, preferred_element_type=jnp.float32
            )[:BAND]
            high, low = split(half)
            both = jnp.dot(high, chigh[...], preferred_element_type=jnp.float32)
            both = both + jnp.dot(low, chigh[...], preferred_element_type=jnp.float32)
            both = both + jnp.dot(high, clow[...], preferred_element_type=jnp.float32)
            bands[0, pl.ds(i * BAND, BAND)] = high_low(both)
            if i < last - 1:
                take_out(i)
        part = pl.ds(first * BAND, (last - first) * BAND)
        n = batches(chunks).index((first, last))
        for t in range(1, nr):
            c = remote(
                bands.at[0, part], bands.at[nr - t, part],
                b_send.at[n, t - 1], b_recv.at[n, nr - t - 1], (lax.rem(r + t, nr), f),
            )
            c.start()
            b_copies.append(c)
        take_out(last - 1)

    for c in w_copies:
        c.wait_recv()
    f_copies = []
    for s in range(pairs - 1):
        q = lax.rem(pair + s + 1, pairs)
        c = remote(wland.at[s], raw_out.at[q * 2 + core], f_send.at[s], f_recv.at[s], partner)
        c.start()
        f_copies.append(c)
        c = pltpu.make_async_copy(wland.at[s], raw_out.at[q * 2 + core], raw_sem.at[s])
        c.start()
        local.append(c)

    for c in b_copies:
        c.wait_recv()
    total = bands[0].astype(jnp.float32)
    for t in range(1, nr):
        total = total + bands[t].astype(jnp.float32)
    means[0] = high_low((total + pltpu.roll(total, HALF, 1)) * (1.0 / nr))
    e_copies = []
    for t in range(1, nf):
        c = remote(
            means.at[0], mean_out.at[f], e_send.at[t - 1], e_recv.at[nf - t - 1],
            (r, lax.rem(f + t, nf)),
        )
        c.start()
        e_copies.append(c)
    c = pltpu.make_async_copy(means.at[0], mean_out.at[f], mean_sem)
    c.start()
    local.append(c)

    for c in local:
        c.wait()
    for c in c_copies + w_copies + b_copies + [c for _, _, c in x_copies]:
        c.wait_send()
    m_copy.wait()
    for c in f_copies + e_copies:
        c.wait()


def finish(nf, taken, master, raw, mean, thigh, tlow, left, f_ref, momentum_out, master_out, full_out, vhigh, vlow):
    width = master.shape[1]
    f = f_ref[0]
    a = pl.program_id(0)

    @pl.when(a == 0)
    def _():
        for j in range(nf):
            vhigh[j], vlow[j] = split(spread_half(mean[j], thigh, tlow))

    momentum_out[...] = taken[...]
    part = pl.ds(pl.multiple_of(a * BAND, BAND), BAND)
    mine = master[...]
    new_master = mine
    for j in range(nf):
        high, low = vhigh[j, part], vlow[j, part]
        delta = jnp.dot(
            left[...], jnp.concatenate([high, high, low], axis=0), preferred_element_type=jnp.float32
        )
        value = jnp.where(f == j, mine, raw[j].astype(jnp.float32)) - step_size * delta
        new_master = jnp.where(f == j, value, new_master)
        full_out[:, j * width : (j + 1) * width] = value.astype(jnp.bfloat16)
    master_out[...] = new_master


def local(nr, nf, gradients, momentum, master_weights):
    rows, width = master_weights.shape
    chunks = rows // GROUP
    pairs = nf // 2
    table, twice = tables(width)
    thigh, tlow = split(twice)
    lhigh, llow = split(table.T)
    left = jnp.concatenate([lhigh, llow, lhigh], axis=1)
    lboth = jnp.concatenate(split(table), axis=0)
    chigh, clow = split(twice.T)
    small = (lboth, chigh, clow, thigh, tlow, left)
    anywhere = pl.BlockSpec(memory_space=pl.ANY)
    dma = pltpu.SemaphoreType.DMA
    bf16, f32 = jnp.bfloat16, jnp.float32
    nb = len(batches(chunks))
    share = rows // nr
    taken, raw, mean = pl.pallas_call(
        functools.partial(exchange, nr, nf),
        out_shape=(
            jax.ShapeDtypeStruct((1, rows, width), f32),
            jax.ShapeDtypeStruct((nf, rows, width), bf16),
            jax.ShapeDtypeStruct((nf, chunks * BAND, LANES), bf16),
        ),
        in_specs=[anywhere] * (3 + len(small)),
        out_specs=(anywhere,) * 3,
        scratch_shapes=[
            pltpu.VMEM((chunks, pairs, GROUP, width), bf16),
            pltpu.VMEM((chunks, pairs, GROUP, width), bf16),
            pltpu.VMEM((chunks, pairs - 1, GROUP, width), bf16),
            pltpu.VMEM((chunks, pairs - 1, GROUP, width), bf16),
            pltpu.VMEM((rows, width), f32),
            pltpu.VMEM((rows, width), f32),
            pltpu.VMEM((2 * rows, width), f32),
            pltpu.VMEM((rows + share, width), bf16),
            pltpu.VMEM((pairs - 1, rows, width), bf16),
            pltpu.VMEM((nr, chunks * BAND, LANES), bf16),
            pltpu.VMEM((1, chunks * BAND, LANES), bf16),
            dma((chunks, pairs)),
            dma((chunks,)),
            dma((2,)),
            dma((chunks,)),
            dma((pairs - 1,)),
            dma,
            dma((chunks, pairs)),
            dma((chunks, pairs)),
            dma((chunks, pairs - 1)),
            dma((chunks, pairs - 1)),
            dma((pairs - 1,)),
            dma((pairs - 1,)),
            dma,
            dma,
            dma((pairs - 1, nr - 1)),
            dma((pairs - 1, nr - 1)),
            dma((pairs - 1,)),
            dma((pairs - 1,)),
            dma((nb, nr - 1)),
            dma((nb, nr - 1)),
            dma((nf - 1,)),
            dma((nf - 1,)),
            dma((len(small),)),
        ]
        + [pltpu.VMEM(t.shape, bf16) for t in small],
        compiler_params=pltpu.CompilerParams(
            collective_id=0, has_side_effects=True, vmem_limit_bytes=60 * 1024 * 1024
        ),
        name="exchange",
    )(gradients, momentum, master_weights, *small)

    def whole(shape):
        return pl.BlockSpec(shape, lambda a: (0,) * len(shape))

    return pl.pallas_call(
        functools.partial(finish, nf),
        grid=(chunks,),
        out_shape=(
            jax.ShapeDtypeStruct((1, rows, width), f32),
            jax.ShapeDtypeStruct((rows, width), f32),
            jax.ShapeDtypeStruct((rows, nf * width), bf16),
        ),
        in_specs=[
            pl.BlockSpec((1, GROUP, width), lambda a: (0, a, 0)),
            pl.BlockSpec((GROUP, width), lambda a: (a, 0)),
            pl.BlockSpec((nf, GROUP, width), lambda a: (0, a, 0)),
            whole((nf, chunks * BAND, LANES)),
            whole((LANES, width)),
            whole((LANES, width)),
            whole((GROUP, 3 * BAND)),
            pl.BlockSpec(memory_space=pltpu.SMEM),
        ],
        out_specs=(
            pl.BlockSpec((1, GROUP, width), lambda a: (0, a, 0)),
            pl.BlockSpec((GROUP, width), lambda a: (a, 0)),
            pl.BlockSpec((GROUP, nf * width), lambda a: (a, 0)),
        ),
        scratch_shapes=[pltpu.VMEM((nf, chunks * BAND, width), bf16)] * 2,
        compiler_params=pltpu.CompilerParams(vmem_limit_bytes=60 * 1024 * 1024),
        name="finish",
    )(taken, master_weights, raw, mean, thigh, tlow, left, lax.axis_index("fsdp").astype(jnp.int32)[None])


def solution(mesh):
    return jax.shard_map(
        functools.partial(local, mesh.shape["rep"], mesh.shape["fsdp"]),
        mesh=mesh,
        in_specs=(P("rep", "fsdp", None, None), P("rep", None, "fsdp"), P(None, "fsdp")),
        out_specs=(P("rep", None, "fsdp"), P(None, "fsdp"), P()),
        check_vma=False,
    )
```
